16 devices in a mesh: dp: 2 (over y, z), sp: 8 (over x, core).
Axes of the slice: x: 4, y: 2, z: 1, core: 2. Of those that a mesh axis runs over, the one named last changes fastest.
The devices are a block of a 4x4x8 slice.
Arguments:
- q: bfloat16 [64, 16, 64], P('dp'), parts along dimension 0
- k: bfloat16 [64, 8192, 16, 64], P('dp', 'sp'), parts along dimension 0
- v: bfloat16 [64, 8192, 16, 64], P('dp', 'sp'), parts along dimension 0
Outputs:
- q: bfloat16 [64, 16, 64], P('dp'), parts along dimension 0
There are 2 independent parts. The reference program is written for one: setup_inputs(seed, part) draws one part's arguments, and reference() takes and returns one part's arrays. A program takes and returns all parts, laid end to end along the dimension named above; each array names one.
All inputs are finite; a program needn't handle non-finite values.
Results may differ from the reference program's by a relative error of at most 0.012.
Values are sent between devices in bfloat16 or wider.
A program may use at most 768 MiB of HBM per device.

```python
import jax
import jax.numpy as jnp

BATCH = 32
CACHE = 8192
HEADS = 16
KV_HEADS = 16
HEAD = 64


def setup_inputs(seed: int = 0, part: int = 0) -> dict:
    kq, kk, kv = (jax.random.fold_in(k, part) for k in jax.random.split(jax.random.key(seed), 3))
    return {
        "q": (3 * jax.random.normal(kq, (BATCH, HEADS, HEAD), jnp.float32)).astype(jnp.bfloat16),
        "k": jax.random.normal(kk, (BATCH, CACHE, KV_HEADS, HEAD), jnp.float32).astype(jnp.bfloat16),
        "v": jax.random.normal(kv, (BATCH, CACHE, KV_HEADS, HEAD), jnp.float32).astype(jnp.bfloat16),
    }


def einsum(form, a, b):
    return jnp.einsum(form, a.astype(jnp.float32), b.astype(jnp.float32))


def reference(q, k, v):
    grouped = q.reshape(BATCH, KV_HEADS, -1, HEAD)
    scores = einsum("bgsd,bugd->bgsu", grouped, k) * HEAD**-0.5
    weights = jax.nn.softmax(scores, -1).astype(jnp.bfloat16)
    return einsum("bgsu,bugd->bgsd", weights, v).astype(jnp.bfloat16).reshape(BATCH, HEADS, HEAD)
```

```python
import functools

import jax
import jax.numpy as jnp
from jax import lax
from jax.experimental import pallas as pl
from jax.experimental.pallas import tpu as pltpu
from jax.sharding import PartitionSpec as P

SLOTS = 5
LAG = 4


def kernel(n, scale, q_ref, k_hbm, v_hbm, out_ref, k_buf, v_buf, parts, k_sem, v_sem, send_sem, recv_sem):
    me = lax.axis_index("sp")
    seqs, heads, head = q_ref.shape
    width = heads * head

    def fetch_k(s, slot):
        return pltpu.make_async_copy(k_hbm.at[s], k_buf.at[slot], k_sem.at[slot])

    def fetch_v(s, slot):
        return pltpu.make_async_copy(v_hbm.at[s], v_buf.at[slot], v_sem.at[slot])

    for s in range(SLOTS):
        fetch_k(s, s).start()
        fetch_v(s, s).start()

    barrier = pltpu.get_barrier_semaphore()
    for d in range(1, n):
        pl.semaphore_signal(barrier, inc=1, device_id={"sp": lax.rem(me + d, n)})

    def weights_of(s, slot):
        q = q_ref[s]
        row = lax.broadcasted_iota(jnp.int32, (heads, width), 0)
        owner = lax.broadcasted_iota(jnp.int32, (heads, width), 1) // head
        diagonal = jnp.where(owner == row, jnp.concatenate([q] * heads, axis=1), jnp.zeros((), q.dtype))
        scores = jnp.dot(diagonal, k_buf[slot], preferred_element_type=jnp.float32) * scale
        high = jnp.max(scores, -1, keepdims=True)
        weights = jnp.exp(scores - high)
        return weights.astype(v_buf.dtype), jnp.sum(weights, -1, keepdims=True), high

    lane = lax.broadcasted_iota(jnp.int32, (heads, 128), 1)
    row = lax.broadcasted_iota(jnp.int32, (heads, 128), 0)

    def part_of(slot, weights, total, high):
        every = lax.dot_general(weights, v_buf[slot], (((1,), (1,)), ((), ())), preferred_element_type=jnp.float32)
        seen = jnp.zeros((heads, 128), jnp.float32)
        per = 128 // head
        for j in range(width // 128):
            seen = jnp.where(lane // head + per * j == row, every[:, 128 * j : 128 * j + 128], seen)
        seen = jnp.where(lane // head == lax.rem(row, per), seen, 0.0)
        seen = seen + pltpu.roll(seen, head, 1)
        return jnp.where(lane < head, seen, jnp.where(lane < head + head // 2, total, high))

    def send(s):
        for d in range(1, n):
            pltpu.make_async_remote_copy(
                src_ref=parts.at[me, s],
                dst_ref=parts.at[me, s],
                send_sem=send_sem,
                recv_sem=recv_sem.at[s],
                device_id={"sp": lax.rem(me + d, n)},
            ).start()

    def combine(s):
        pltpu.make_async_copy(parts.at[pl.ds(0, n - 1), s], parts.at[pl.ds(0, n - 1), s], recv_sem.at[s]).wait()
        tiles = [parts[p, s] for p in range(n)]
        highs = [jnp.broadcast_to(t[:, 127:128], t.shape) for t in tiles]
        top = functools.reduce(jnp.maximum, highs)
        both = functools.reduce(jnp.add, [t * jnp.exp(h - top) for t, h in zip(tiles, highs)])
        out_ref[s] = (both / jnp.broadcast_to(both[:, head : head + 1], both.shape))[:, :head].astype(out_ref.dtype)

    fetch_k(0, 0).wait()
    state = weights_of(0, 0)
    pl.semaphore_wait(barrier, n - 1)

    def step(s, state):
        slot, before = lax.rem(s, SLOTS), lax.rem(s - 1, SLOTS)
        fetch_k(s, slot).wait()
        fetch_v(s - 1, before).wait()
        parts[me, s - 1] = part_of(before, *state)
        state = weights_of(s, slot)

        @pl.when(s - 1 + SLOTS < seqs)
        def _():
            fetch_v(s - 1 + SLOTS, before).start()

        @pl.when(s + SLOTS < seqs)
        def _():
            fetch_k(s + SLOTS, slot).start()

        send(s - 1)

        @pl.when(s > LAG)
        def _():
            combine(s - 1 - LAG)

        return state

    fetch_k(SLOTS, 0).start()
    state = lax.fori_loop(1, seqs, step, state)

    last = seqs - 1
    fetch_v(last, last % SLOTS).wait()
    parts[me, last] = part_of(last % SLOTS, *state)
    send(last)
    for s in range(seqs - 1 - LAG, seqs):
        combine(s)
    pltpu.make_async_copy(parts.at[pl.ds(0, n - 1)], parts.at[pl.ds(0, n - 1)], send_sem).wait()


def solution(mesh):
    n = mesh.shape["sp"]

    def step(q, k, v):
        seqs, tokens, heads, head = k.shape
        k = jnp.transpose(k, (0, 2, 3, 1)).reshape(seqs, heads * head, tokens)
        v = jnp.transpose(v, (0, 2, 3, 1)).reshape(seqs, heads * head, tokens)
        return pl.pallas_call(
            functools.partial(kernel, n, head**-0.5),
            out_shape=jax.ShapeDtypeStruct(q.shape, q.dtype),
            in_specs=[
                pl.BlockSpec(memory_space=pltpu.VMEM),
                pl.BlockSpec(memory_space=pl.ANY),
                pl.BlockSpec(memory_space=pl.ANY),
            ],
            out_specs=pl.BlockSpec(memory_space=pltpu.VMEM),
            scratch_shapes=[
                pltpu.VMEM((SLOTS, heads * head, tokens), k.dtype),
                pltpu.VMEM((SLOTS, heads * head, tokens), v.dtype),
                pltpu.VMEM((n, seqs, heads, 128), jnp.float32),
                pltpu.SemaphoreType.DMA((SLOTS,)),
                pltpu.SemaphoreType.DMA((SLOTS,)),
                pltpu.SemaphoreType.DMA,
                pltpu.SemaphoreType.DMA((seqs,)),
            ],
            compiler_params=pltpu.CompilerParams(collective_id=0, has_side_effects=True, vmem_limit_bytes=60 * 1024 * 1024),
            cost_estimate=pl.CostEstimate(
                flops=4 * seqs * tokens * heads * head,
                bytes_accessed=2 * k.size * k.dtype.itemsize,
                transcendentals=seqs * heads * tokens,
            ),
        )(q, k, v)

    return jax.shard_map(
        step,
        mesh=mesh,
        in_specs=(P("dp", None, None), P("dp", "sp", None, None), P("dp", "sp", None, None)),
        out_specs=P("dp", None, None),
        check_vma=False,
    )
```

```python
import functools

import jax
import jax.numpy as jnp
from jax import lax
from jax.experimental import pallas as pl
from jax.experimental.pallas import tpu as pltpu
from jax.sharding import PartitionSpec as P

SLOTS = 4
LAG = 4


def kernel(n, scale, q_hbm, k_hbm, v_hbm, out_ref, q_ref, k_buf, v_buf, parts, q_sem, k_sem, v_sem, send_sem, recv_sem):
    me = lax.axis_index("sp")
    seqs, heads, head = q_ref.shape
    width = heads * head

    def fetch_k(s, slot):
        return pltpu.make_async_copy(k_hbm.at[s], k_buf.at[slot], k_sem.at[slot])

    def fetch_v(s, slot):
        return pltpu.make_async_copy(v_hbm.at[s], v_buf.at[slot], v_sem.at[slot])

    fetch_q = pltpu.make_async_copy(q_hbm, q_ref, q_sem)
    fetch_q.start()
    for s in range(SLOTS):
        fetch_k(s, s).start(priority=1)
        fetch_v(s, s).start(priority=1)

    barrier = pltpu.get_barrier_semaphore()
    for d in range(1, n):
        pl.semaphore_signal(barrier, inc=1, device_id={"sp": lax.rem(me + d, n)})

    def weights_of(s, slot):
        q = q_ref[s]
        row = lax.broadcasted_iota(jnp.int32, (heads, width), 0)
        owner = lax.broadcasted_iota(jnp.int32, (heads, width), 1) // head
        diagonal = jnp.where(owner == row, jnp.concatenate([q] * heads, axis=1), jnp.zeros((), q.dtype))
        scores = jnp.dot(diagonal, k_buf[slot], preferred_element_type=jnp.float32) * scale
        high = jnp.max(scores, -1, keepdims=True)
        weights = jnp.exp(scores - high)
        return weights.astype(v_buf.dtype), jnp.sum(weights, -1, keepdims=True), high

    lane = lax.broadcasted_iota(jnp.int32, (heads, 128), 1)
    row = lax.broadcasted_iota(jnp.int32, (heads, 128), 0)
    per = 128 // head

    def part_of(slot, weights, total, high):
        every = lax.dot_general(weights, v_buf[slot], (((1,), (1,)), ((), ())), preferred_element_type=jnp.float32)
        seen = jnp.zeros((heads, 128), jnp.float32)
        for j in range(width // 128):
            seen = jnp.where(lane // head + per * j == row, every[:, 128 * j : 128 * j + 128], seen)
        seen = seen + pltpu.roll(seen, head, 1)
        return jnp.where(lane < head, seen, jnp.where(lane < head + head // 2, total, high))

    def send(s):
        place = parts.at[me, s]
        for d in sorted(range(1, n), key=lambda d: -min(d, n - d)):
            pltpu.make_async_remote_copy(
                src_ref=place,
                dst_ref=place,
                send_sem=send_sem,
                recv_sem=recv_sem.at[s],
                device_id={"sp": lax.rem(me + d, n)},
            ).start()

    def wait_parts(s):
        place = parts.at[pl.ds(0, n - 1), s]
        pltpu.make_async_copy(place, place, recv_sem.at[s]).wait()

    def combine(s):
        tiles = [parts[p, s] for p in range(n)]
        highs = [jnp.broadcast_to(t[:, 127:128], t.shape) for t in tiles]
        top = functools.reduce(jnp.maximum, highs)
        both = functools.reduce(jnp.add, [t * jnp.exp(h - top) for t, h in zip(tiles, highs)])
        result = both / jnp.broadcast_to(both[:, head : head + 1], both.shape)
        out_ref[s] = result[:, :head].astype(out_ref.dtype)

    def block(s, state):
        slot, after = lax.rem(s, SLOTS), lax.rem(s + 1, SLOTS)
        coming = weights_of(s + 1, after)
        parts[me, s] = part_of(slot, *state)

        @pl.when(s + SLOTS < seqs)
        def _():
            fetch_v(s + SLOTS, slot).start(priority=1)

        @pl.when(s + 1 + SLOTS < seqs)
        def _():
            fetch_k(s + 1 + SLOTS, after).start(priority=1)

        return coming

    def need(s):
        fetch_k(s + 1, lax.rem(s + 1, SLOTS)).wait()
        fetch_v(s, lax.rem(s, SLOTS)).wait()

    fetch_q.wait()
    fetch_k(0, 0).wait()
    state = weights_of(0, 0)
    fetch_k(SLOTS, 0).start(priority=1)
    pl.semaphore_wait(barrier, n - 1)
    need(0)
    state = block(0, state)

    def early(s, state):
        need(s)
        send(s - 1)
        return block(s, state)

    def later(s, state):
        wait_parts(s - 1 - LAG)
        need(s)
        send(s - 1)
        combine(s - 1 - LAG)
        return block(s, state)

    last = seqs - 1
    state = lax.fori_loop(1, 1 + LAG, early, state)
    state = lax.fori_loop(1 + LAG, last - 1, later, state)

    send(last - 2)
    fetch_v(last - 1, (last - 1) % SLOTS).wait()
    parts[me, last - 1] = part_of((last - 1) % SLOTS, *state)
    fetch_k(last, last % SLOTS).wait()
    state = weights_of(last, last % SLOTS)
    send(last - 1)
    fetch_v(last, last % SLOTS).wait()
    parts[me, last] = part_of(last % SLOTS, *state)
    send(last)
    for s in range(last - 2 - LAG, seqs):
        wait_parts(s)
        combine(s)
    pltpu.make_async_copy(parts.at[pl.ds(0, n - 1)], parts.at[pl.ds(0, n - 1)], send_sem).wait()


def solution(mesh):
    n = mesh.shape["sp"]

    def step(q, k, v):
        seqs, tokens, heads, head = k.shape
        k = jnp.transpose(k, (0, 2, 3, 1)).reshape(seqs, heads * head, tokens)
        v = jnp.transpose(v, (0, 2, 3, 1)).reshape(seqs, heads * head, tokens)
        return pl.pallas_call(
            functools.partial(kernel, n, head**-0.5),
            out_shape=jax.ShapeDtypeStruct(q.shape, q.dtype),
            in_specs=[pl.BlockSpec(memory_space=pl.ANY)] * 3,
            out_specs=pl.BlockSpec(memory_space=pltpu.VMEM),
            scratch_shapes=[
                pltpu.VMEM(q.shape, q.dtype),
                pltpu.VMEM((SLOTS, heads * head, tokens), k.dtype),
                pltpu.VMEM((SLOTS, heads * head, tokens), v.dtype),
                pltpu.VMEM((n, seqs, heads, 128), jnp.float32),
                pltpu.SemaphoreType.DMA,
                pltpu.SemaphoreType.DMA((SLOTS,)),
                pltpu.SemaphoreType.DMA((SLOTS,)),
                pltpu.SemaphoreType.DMA,
                pltpu.SemaphoreType.DMA((seqs,)),
            ],
            compiler_params=pltpu.CompilerParams(
                collective_id=0, has_side_effects=True, vmem_limit_bytes=30 * 1024 * 1024
            ),
            cost_estimate=pl.CostEstimate(
                flops=4 * seqs * tokens * heads * head,
                bytes_accessed=2 * k.size * k.dtype.itemsize,
                transcendentals=seqs * heads * tokens,
            ),
        )(pltpu.with_memory_space_constraint(q, pltpu.HBM), k, v)

    return jax.shard_map(
        step,
        mesh=mesh,
        in_specs=(P("dp", None, None), P("dp", "sp", None, None), P("dp", "sp", None, None)),
        out_specs=P("dp", None, None),
        check_vma=False,
    )
```

```python
import functools

import jax
import jax.numpy as jnp
from jax import lax
from jax.experimental import pallas as pl
from jax.experimental.pallas import tpu as pltpu
from jax.sharding import PartitionSpec as P

SLOTS = 4
ASIDE = 8
LAG = 4


def kernel(n, scale, q_hbm, k_hbm, v_hbm, out_ref, q_ref, k_buf, v_buf, parts, q_sem, k_sem, v_sem, send_sem, recv_sem):
    me = lax.axis_index("sp")
    seqs, heads, head = q_ref.shape
    width = heads * head

    def fetch_k(s, slot):
        return pltpu.make_async_copy(k_hbm.at[s], k_buf.at[slot], k_sem.at[slot])

    def fetch_v(s, slot):
        return pltpu.make_async_copy(v_hbm.at[s], v_buf.at[slot], v_sem.at[slot])

    fetch_q = pltpu.make_async_copy(q_hbm, q_ref, q_sem)
    fetch_q.start()
    fetch_k(0, 0).start(priority=1)
    for s in range(1, SLOTS):
        fetch_k(s, s).start(priority=1)
        fetch_v(s - 1, s - 1).start(priority=1)

    barrier = pltpu.get_barrier_semaphore()
    for d in range(1, n):
        pl.semaphore_signal(barrier, inc=1, device_id={"sp": lax.rem(me + d, n)})

    def weights_of(s, slot):
        q = q_ref[s]
        row = lax.broadcasted_iota(jnp.int32, (heads, width), 0)
        owner = lax.broadcasted_iota(jnp.int32, (heads, width), 1) // head
        diagonal = jnp.where(owner == row, jnp.concatenate([q] * heads, axis=1), jnp.zeros((), q.dtype))
        scores = jnp.dot(diagonal, k_buf[slot], preferred_element_type=jnp.float32) * scale
        high = jnp.max(scores, -1, keepdims=True)
        weights = jnp.exp(scores - high)
        return weights.astype(v_buf.dtype), jnp.sum(weights, -1, keepdims=True), high

    lane = lax.broadcasted_iota(jnp.int32, (heads, 128), 1)
    row = lax.broadcasted_iota(jnp.int32, (heads, 128), 0)
    per = 128 // head

    def part_of(slot, weights, total, high):
        cut = (heads - ASIDE) * head
        every = lax.dot_general(weights, v_buf[slot, :cut], (((1,), (1,)), ((), ())), preferred_element_type=jnp.float32)
        seen = jnp.zeros((heads, 128), jnp.float32)
        for j in range(cut // 128):
            seen = jnp.where(lane // head + per * j == row, every[:, 128 * j : 128 * j + 128], seen)
        seen = seen + pltpu.roll(seen, head, 1)
        wide = weights.astype(jnp.float32)
        column = lax.broadcasted_iota(jnp.int32, (head, 128), 1)
        turned = jnp.zeros((head, 128), jnp.float32)
        for h in range(heads - ASIDE, heads):
            terms = [
                v_buf[slot, h * head : (h + 1) * head, t : t + 128].astype(jnp.float32) * wide[h : h + 1, t : t + 128]
                for t in range(0, wide.shape[1], 128)
            ]
            turned = jnp.where(column == h, jnp.sum(functools.reduce(jnp.add, terms), 1, keepdims=True), turned)
        turned = turned.T[:heads]
        seen = seen + jnp.concatenate([turned, turned], 1)
        return jnp.where(lane < head, seen, jnp.where(lane < head + head // 2, total, high))

    def send(s):
        place = parts.at[me, s]
        for d in sorted(range(1, n), key=lambda d: -min(d, n - d)):
            pltpu.make_async_remote_copy(
                src_ref=place,
                dst_ref=place,
                send_sem=send_sem,
                recv_sem=recv_sem.at[s],
                device_id={"sp": lax.rem(me + d, n)},
            ).start()

    def wait_parts(s):
        place = parts.at[pl.ds(0, n - 1), s]
        pltpu.make_async_copy(place, place, recv_sem.at[s]).wait()

    def combine(s):
        tiles = [parts[p, s] for p in range(n)]
        highs = [jnp.broadcast_to(t[:, 127:128], t.shape) for t in tiles]
        top = functools.reduce(jnp.maximum, highs)
        both = functools.reduce(jnp.add, [t * jnp.exp(h - top) for t, h in zip(tiles, highs)])
        result = both / jnp.broadcast_to(both[:, head : head + 1], both.shape)
        out_ref[s] = result[:, :head].astype(out_ref.dtype)

    def block(s, state):
        slot, after = lax.rem(s, SLOTS), lax.rem(s + 1, SLOTS)
        coming = weights_of(s + 1, after)
        parts[me, s] = part_of(slot, *state)

        @pl.when(s + 1 + SLOTS < seqs)
        def _():
            fetch_k(s + 1 + SLOTS, after).start(priority=1)

        @pl.when(s + SLOTS < seqs)
        def _():
            fetch_v(s + SLOTS, slot).start(priority=1)

        return coming

    def need(s):
        fetch_k(s + 1, lax.rem(s + 1, SLOTS)).wait()
        fetch_v(s, lax.rem(s, SLOTS)).wait()

    fetch_q.wait()
    fetch_k(0, 0).wait()
    state = weights_of(0, 0)
    fetch_k(SLOTS, 0).start(priority=1)
    fetch_v(SLOTS - 1, SLOTS - 1).start(priority=1)
    pl.semaphore_wait(barrier, n - 1)
    need(0)
    state = block(0, state)

    def early(s, state):
        need(s)
        send(s - 1)
        return block(s, state)

    def later(s, state):
        wait_parts(s - 1 - LAG)
        need(s)
        send(s - 1)
        combine(s - 1 - LAG)
        return block(s, state)

    last = seqs - 1
    state = lax.fori_loop(1, 1 + LAG, early, state)
    state = lax.fori_loop(1 + LAG, last - 1, later, state)

    send(last - 2)
    fetch_k(last, last % SLOTS).wait()
    coming = weights_of(last, last % SLOTS)
    fetch_v(last - 1, (last - 1) % SLOTS).wait()
    parts[me, last - 1] = part_of((last - 1) % SLOTS, *state)
    state = coming
    send(last - 1)
    fetch_v(last, last % SLOTS).wait()
    parts[me, last] = part_of(last % SLOTS, *state)
    send(last)
    for s in range(last - 2 - LAG, seqs):
        wait_parts(s)
        combine(s)
    pltpu.make_async_copy(parts.at[pl.ds(0, n - 1)], parts.at[pl.ds(0, n - 1)], send_sem).wait()


def solution(mesh):
    n = mesh.shape["sp"]

    def step(q, k, v):
        seqs, tokens, heads, head = k.shape
        k = jnp.transpose(k, (0, 2, 3, 1)).reshape(seqs, heads * head, tokens)
        v = jnp.transpose(v, (0, 2, 3, 1)).reshape(seqs, heads * head, tokens)
        return pl.pallas_call(
            functools.partial(kernel, n, head**-0.5),
            out_shape=jax.ShapeDtypeStruct(q.shape, q.dtype),
            in_specs=[pl.BlockSpec(memory_space=pl.ANY)] * 3,
            out_specs=pl.BlockSpec(memory_space=pltpu.VMEM),
            scratch_shapes=[
                pltpu.VMEM(q.shape, q.dtype),
                pltpu.VMEM((SLOTS, heads * head, tokens), k.dtype),
                pltpu.VMEM((SLOTS, heads * head, tokens), v.dtype),
                pltpu.VMEM((n, seqs, heads, 128), jnp.float32),
                pltpu.SemaphoreType.DMA,
                pltpu.SemaphoreType.DMA((SLOTS,)),
                pltpu.SemaphoreType.DMA((SLOTS,)),
                pltpu.SemaphoreType.DMA,
                pltpu.SemaphoreType.DMA((seqs,)),
            ],
            compiler_params=pltpu.CompilerParams(
                collective_id=0, has_side_effects=True, vmem_limit_bytes=30 * 1024 * 1024
            ),
            cost_estimate=pl.CostEstimate(
                flops=4 * seqs * tokens * heads * head,
                bytes_accessed=2 * k.size * k.dtype.itemsize,
                transcendentals=seqs * heads * tokens,
            ),
        )(pltpu.with_memory_space_constraint(q, pltpu.HBM), k, v)

    return jax.shard_map(
        step,
        mesh=mesh,
        in_specs=(P("dp", None, None), P("dp", "sp", None, None), P("dp", "sp", None, None)),
        out_specs=P("dp", None, None),
        check_vma=False,
    )
```

```python
import functools

import jax
import jax.numpy as jnp
from jax import lax
from jax.experimental import pallas as pl
from jax.experimental.pallas import tpu as pltpu
from jax.sharding import PartitionSpec as P

SLOTS = 3
ASIDE = 8
LAG = 7
BATCH = 4


def kernel(n, scale, q_hbm, k_hbm, v_hbm, out_ref, q_ref, k_buf, v_buf, parts, q_sem, k_sem, v_sem, send_sem, recv_sem):
    me = lax.axis_index("sp")
    seqs, heads, head = q_ref.shape
    width = heads * head
    last = seqs - 1

    def fetch_k(s):
        slot = lax.rem(s, SLOTS)
        return pltpu.make_async_copy(k_hbm.at[s], k_buf.at[slot], k_sem.at[slot])

    def fetch_v(s):
        slot = lax.rem(s, SLOTS)
        return pltpu.make_async_copy(v_hbm.at[s], v_buf.at[slot], v_sem.at[slot])

    for copy in fetch_k(0), fetch_k(1), fetch_v(0), fetch_k(2), fetch_v(1):
        copy.start(priority=1)
    fetch_q = pltpu.make_async_copy(q_hbm, q_ref, q_sem)
    fetch_q.start()

    barrier = pltpu.get_barrier_semaphore()
    for d in range(1, n):
        pl.semaphore_signal(barrier, inc=1, device_id={"sp": lax.rem(me + d, n)})

    def need(s):
        fetch_k(s + 1).wait()

        @pl.when(s + 3 < seqs)
        def _():
            fetch_k(s + 3).start(priority=1)

        fetch_v(s).wait()

        @pl.when(s + 2 < seqs)
        def _():
            fetch_v(s + 2).start(priority=1)

    def weights_of(s):
        q = q_ref[s]
        row = lax.broadcasted_iota(jnp.int32, (heads, width), 0)
        owner = lax.broadcasted_iota(jnp.int32, (heads, width), 1) // head
        diagonal = jnp.where(owner == row, jnp.concatenate([q] * heads, axis=1), jnp.zeros((), q.dtype))
        scores = jnp.dot(diagonal, k_buf[lax.rem(s, SLOTS)], preferred_element_type=jnp.float32) * scale
        high = jnp.max(scores, -1, keepdims=True)
        weights = jnp.exp(scores - high)
        return weights.astype(v_buf.dtype), jnp.sum(weights, -1, keepdims=True), high

    lane = lax.broadcasted_iota(jnp.int32, (heads, 128), 1)
    row = lax.broadcasted_iota(jnp.int32, (heads, 128), 0)
    per = 128 // head

    def seen_of(s, weights):
        slot, cut = lax.rem(s, SLOTS), (heads - ASIDE) * head
        every = lax.dot_general(
            weights, v_buf[slot, :cut], (((1,), (1,)), ((), ())), preferred_element_type=jnp.float32
        )
        seen = jnp.zeros((heads, 128), jnp.float32)
        for j in range(cut // 128):
            seen = jnp.where(lane // head + per * j == row, every[:, 128 * j : 128 * j + 128], seen)
        seen = seen + pltpu.roll(seen, head, 1)
        wide = weights.astype(jnp.float32)
        column = lax.broadcasted_iota(jnp.int32, (head, 128), 1)
        turned = jnp.zeros((head, 128), jnp.float32)
        for h in range(heads - ASIDE, heads):
            terms = [
                v_buf[slot, h * head : (h + 1) * head, t : t + 128].astype(jnp.float32) * wide[h : h + 1, t : t + 128]
                for t in range(0, wide.shape[1], 128)
            ]
            turned = jnp.where(column == h, jnp.sum(functools.reduce(jnp.add, terms), 1, keepdims=True), turned)
        turned = turned.T[:heads]
        return seen + jnp.concatenate([turned, turned], 1)

    def place_of(s, count=1):
        return parts.at[me, pl.ds(s, count)]

    def sem_of(s):
        return recv_sem.at[jnp.maximum(s // BATCH, s - (seqs - BATCH) + seqs // BATCH - 1)]

    def send(s):
        for d in sorted(range(1, n), key=lambda d: -min(d, n - d)):
            pltpu.make_async_remote_copy(
                src_ref=parts.at[me, s],
                dst_ref=parts.at[me, s],
                send_sem=send_sem,
                recv_sem=sem_of(s),
                device_id={"sp": lax.rem(me + d, n)},
            ).start()

    def wait_parts(s, count=1):
        place = parts.at[pl.ds(0, n - 1), pl.ds(s, count)]
        pltpu.make_async_copy(place, place, sem_of(s)).wait()

    def shares(tiles, total, high):
        highs = [jnp.broadcast_to(t[:, high : high + 1], t.shape) for t in tiles]
        top = functools.reduce(jnp.maximum, highs)
        factors = [jnp.exp(h - top) for h in highs]
        sums = [f * t for f, t in zip(factors, tiles)]
        whole = functools.reduce(jnp.add, sums)
        return factors, whole, jnp.broadcast_to(whole[:, total : total + 1], whole.shape)

    run = head // 4

    def combine(s):
        _, whole, total = shares([parts[p, s] for p in range(n)], head, head + run)
        out_ref[s] = (whole / total)[:, :head].astype(out_ref.dtype)

    def block(s, state):
        weights, total, high = state
        coming = weights_of(s + 1)
        lanes = seen_of(s, weights)
        for first, value in zip(range(head, 2 * head, run), (total, high, coming[1], coming[2])):
            lanes = jnp.where(lane < first, lanes, value)
        parts[me, s] = lanes
        return coming

    def early(s, state):
        need(s)
        state = block(s, state)
        send(s)
        return state

    def later(s, state):
        done = s - 1 - LAG

        @pl.when(lax.rem(done, BATCH) == 0)
        def _():
            wait_parts(done, BATCH)

        need(s)
        combine(done)
        state = block(s, state)
        send(s)
        return state

    fetch_q.wait()
    fetch_k(0).wait()
    state = weights_of(0)
    pl.semaphore_wait(barrier, n - 1)
    state = lax.fori_loop(0, 1 + LAG, early, state)
    state = lax.fori_loop(1 + LAG, last, later, state)

    fetch_v(last).wait()
    parts[me, last] = seen_of(last, state[0])
    send(last)
    for s in range(last - 1 - LAG, last):
        if s >= seqs - BATCH:
            wait_parts(s)
        elif s % BATCH == 0:
            wait_parts(s, BATCH)
        combine(s)
    factors, _, total = shares([parts[p, last - 1] for p in range(n)], head + 2 * run, head + 3 * run)
    factors = [f / total for f in factors]
    wait_parts(last)
    whole = functools.reduce(jnp.add, [f * parts[p, last] for p, f in enumerate(factors)])
    out_ref[last] = whole[:, :head].astype(out_ref.dtype)
    pltpu.make_async_copy(parts.at[pl.ds(0, n - 1)], parts.at[pl.ds(0, n - 1)], send_sem).wait()


def solution(mesh):
    n = mesh.shape["sp"]

    def step(q, k, v):
        seqs, tokens, heads, head = k.shape
        k = jnp.transpose(k, (0, 2, 3, 1)).reshape(seqs, heads * head, tokens)
        v = jnp.transpose(v, (0, 2, 3, 1)).reshape(seqs, heads * head, tokens)
        return pl.pallas_call(
            functools.partial(kernel, n, head**-0.5),
            out_shape=jax.ShapeDtypeStruct(q.shape, q.dtype),
            in_specs=[pl.BlockSpec(memory_space=pl.ANY)] * 3,
            out_specs=pl.BlockSpec(memory_space=pltpu.VMEM),
            scratch_shapes=[
                pltpu.VMEM(q.shape, q.dtype),
                pltpu.VMEM((SLOTS, heads * head, tokens), k.dtype),
                pltpu.VMEM((SLOTS, heads * head, tokens), v.dtype),
                pltpu.VMEM((n, seqs, heads, 128), jnp.float32),
                pltpu.SemaphoreType.DMA,
                pltpu.SemaphoreType.DMA((SLOTS,)),
                pltpu.SemaphoreType.DMA((SLOTS,)),
                pltpu.SemaphoreType.DMA,
                pltpu.SemaphoreType.DMA((seqs // BATCH - 1 + BATCH,)),
            ],
            compiler_params=pltpu.CompilerParams(
                collective_id=0, has_side_effects=True, vmem_limit_bytes=30 * 1024 * 1024
            ),
            cost_estimate=pl.CostEstimate(
                flops=4 * seqs * tokens * heads * head,
                bytes_accessed=2 * k.size * k.dtype.itemsize,
                transcendentals=seqs * heads * tokens,
            ),
        )(pltpu.with_memory_space_constraint(q, pltpu.HBM), k, v)

    return jax.shard_map(
        step,
        mesh=mesh,
        in_specs=(P("dp", None, None), P("dp", "sp", None, None), P("dp", "sp", None, None)),
        out_specs=P("dp", None, None),
        check_vma=False,
    )
```

```python
import functools

import jax
import jax.numpy as jnp
from jax import lax
from jax.experimental import pallas as pl
from jax.experimental.pallas import tpu as pltpu
from jax.sharding import PartitionSpec as P

SLOTS = 3
ASIDE = 8
LAG = 9
BATCH = 6
ALONE = 2


def kernel(n, scale, q_hbm, k_hbm, v_hbm, out_ref, q_ref, k_buf, v_buf, parts, q_sem, k_sem, v_sem, send_sem, recv_sem):
    me = lax.axis_index("sp")
    seqs, heads, head = q_ref.shape
    width = heads * head
    last = seqs - 1
    cut = (heads - ASIDE) * head

    def fetch(hbm, buf, sem, s, piece):
        rows = width // sem.shape[1]
        slot, place = lax.rem(s, SLOTS), pl.ds(piece * rows, rows)
        return pltpu.make_async_copy(hbm.at[s, place], buf.at[slot, place], sem.at[slot, piece])

    fetch_k = [functools.partial(fetch, k_hbm, k_buf, k_sem, piece=p) for p in range(k_sem.shape[1])]
    fetch_v = [functools.partial(fetch, v_hbm, v_buf, v_sem, piece=p) for p in range(v_sem.shape[1])]

    for s, copies in (0, fetch_k), (1, fetch_k), (0, fetch_v), (2, fetch_k), (1, fetch_v):
        for copy in copies:
            copy(s).start(priority=1)
    fetch_q = pltpu.make_async_copy(q_hbm, q_ref, q_sem)
    fetch_q.start()

    barrier = pltpu.get_barrier_semaphore()
    for d in range(1, n):
        pl.semaphore_signal(barrier, inc=1, device_id={"sp": lax.rem(me + d, n)})

    def turn(s, fetch, ahead):
        fetch(s).wait()

        @pl.when(s + ahead < seqs)
        def _():
            fetch(s + ahead).start(priority=1)

    def scores_of(s):
        q = q_ref[s]
        row = lax.broadcasted_iota(jnp.int32, (heads, width), 0)
        owner = lax.broadcasted_iota(jnp.int32, (heads, width), 1) // head
        diagonal = jnp.where(owner == row, jnp.concatenate([q] * heads, axis=1), jnp.zeros((), q.dtype))
        return jnp.dot(diagonal, k_buf[lax.rem(s, SLOTS)], preferred_element_type=jnp.float32) * scale

    def weights_of(scores):
        high = jnp.max(scores, -1, keepdims=True)
        weights = jnp.exp(scores - high)
        return weights.astype(v_buf.dtype), jnp.sum(weights, -1, keepdims=True), high

    lane = lax.broadcasted_iota(jnp.int32, (heads, 128), 1)
    row = lax.broadcasted_iota(jnp.int32, (heads, 128), 0)
    per = 128 // head

    def low_of(s, weights):
        every = lax.dot_general(
            weights, v_buf[lax.rem(s, SLOTS), :cut], (((1,), (1,)), ((), ())), preferred_element_type=jnp.float32
        )
        seen = jnp.zeros((heads, 128), jnp.float32)
        for j in range(cut // 128):
            seen = jnp.where(lane // head + per * j == row, every[:, 128 * j : 128 * j + 128], seen)
        return seen + pltpu.roll(seen, head, 1)

    def high_of(s, weights):
        slot = lax.rem(s, SLOTS)
        wide = weights.astype(jnp.float32)
        column = lax.broadcasted_iota(jnp.int32, (head, 128), 1)
        turned = jnp.zeros((head, 128), jnp.float32)
        for h in range(heads - ASIDE, heads):
            terms = [
                v_buf[slot, h * head : (h + 1) * head, t : t + 128].astype(jnp.float32) * wide[h : h + 1, t : t + 128]
                for t in range(0, wide.shape[1], 128)
            ]
            turned = jnp.where(column == h, jnp.sum(functools.reduce(jnp.add, terms), 1, keepdims=True), turned)
        turned = turned.T[:heads]
        return jnp.concatenate([turned, turned], 1)

    def sem_of(s):
        return recv_sem.at[jnp.maximum(s // BATCH, s - (seqs - ALONE) + (seqs - ALONE) // BATCH)]

    def send(s):
        for d in sorted(range(1, n), key=lambda d: -min(d, n - d)):
            pltpu.make_async_remote_copy(
                src_ref=parts.at[me, s],
                dst_ref=parts.at[me, s],
                send_sem=send_sem,
                recv_sem=sem_of(s),
                device_id={"sp": lax.rem(me + d, n)},
            ).start()

    def wait_parts(s, count=1):
        place = parts.at[pl.ds(0, n - 1), pl.ds(s, count)]
        pltpu.make_async_copy(place, place, sem_of(s)).wait()

    def shares(tiles, total, high):
        highs = [jnp.broadcast_to(t[:, high : high + 1], t.shape) for t in tiles]
        top = functools.reduce(jnp.maximum, highs)
        factors = [jnp.exp(h - top) for h in highs]
        sums = [f * t for f, t in zip(factors, tiles)]
        whole = functools.reduce(jnp.add, sums)
        return factors, whole, jnp.broadcast_to(whole[:, total : total + 1], whole.shape)

    run = head // 4

    def combine(s):
        _, whole, total = shares([parts[p, s] for p in range(n)], head, head + run)
        out_ref[s] = (whole / total)[:, :head].astype(out_ref.dtype)

    def block(s, state, done=None):
        weights, total, high = state
        for copy in fetch_k:
            turn(s + 1, copy, 2)
        scores = scores_of(s + 1)
        if done is not None:
            combine(done)
        for copy in fetch_v:
            turn(s, copy, 2)
        seen = high_of(s, weights)
        coming = weights_of(scores)
        lanes = low_of(s, weights) + seen
        for first, value in zip(range(head, 2 * head, run), (total, high, coming[1], coming[2])):
            lanes = jnp.where(lane < first, lanes, value)
        parts[me, s] = lanes
        send(s)
        return coming

    def later(s, state):
        done = s - 1 - LAG

        @pl.when(lax.rem(done, BATCH) == 0)
        def _():
            wait_parts(done, BATCH)

        return block(s, state, done)

    fetch_q.wait()
    for copy in fetch_k:
        copy(0).wait()
    state = weights_of(scores_of(0))
    pl.semaphore_wait(barrier, n - 1)
    state = lax.fori_loop(0, 1 + LAG, block, state)
    state = lax.fori_loop(1 + LAG, last, later, state)

    for copy in fetch_v:
        copy(last).wait()
    seen = high_of(last, state[0])
    parts[me, last] = seen + low_of(last, state[0])
    send(last)
    for s in range(last - 1 - LAG, last):
        if s >= seqs - ALONE:
            wait_parts(s)
        elif s % BATCH == 0:
            wait_parts(s, BATCH)
        combine(s)
    factors, _, total = shares([parts[p, last - 1] for p in range(n)], head + 2 * run, head + 3 * run)
    factors = [f / total for f in factors]
    wait_parts(last)
    whole = functools.reduce(jnp.add, [f * parts[p, last] for p, f in enumerate(factors)])
    out_ref[last] = whole[:, :head].astype(out_ref.dtype)
    pltpu.make_async_copy(parts.at[pl.ds(0, n - 1)], parts.at[pl.ds(0, n - 1)], send_sem).wait()


def solution(mesh):
    n = mesh.shape["sp"]

    def step(q, k, v):
        seqs, tokens, heads, head = k.shape
        k = jnp.transpose(k, (0, 2, 3, 1)).reshape(seqs, heads * head, tokens)
        v = jnp.transpose(v, (0, 2, 3, 1)).reshape(seqs, heads * head, tokens)
        return pl.pallas_call(
            functools.partial(kernel, n, head**-0.5),
            out_shape=jax.ShapeDtypeStruct(q.shape, q.dtype),
            in_specs=[pl.BlockSpec(memory_space=pl.ANY)] * 3,
            out_specs=pl.BlockSpec(memory_space=pltpu.VMEM),
            scratch_shapes=[
                pltpu.VMEM(q.shape, q.dtype),
                pltpu.VMEM((SLOTS, heads * head, tokens), k.dtype),
                pltpu.VMEM((SLOTS, heads * head, tokens), v.dtype),
                pltpu.VMEM((n, seqs, heads, 128), jnp.float32),
                pltpu.SemaphoreType.DMA,
                pltpu.SemaphoreType.DMA((SLOTS, 1)),
                pltpu.SemaphoreType.DMA((SLOTS, 2)),
                pltpu.SemaphoreType.DMA,
                pltpu.SemaphoreType.DMA(((seqs - ALONE) // BATCH + ALONE,)),
            ],
            compiler_params=pltpu.CompilerParams(
                collective_id=0, has_side_effects=True, vmem_limit_bytes=30 * 1024 * 1024
            ),
            cost_estimate=pl.CostEstimate(
                flops=4 * seqs * tokens * heads * head,
                bytes_accessed=2 * k.size * k.dtype.itemsize,
                transcendentals=seqs * heads * tokens,
            ),
        )(pltpu.with_memory_space_constraint(q, pltpu.HBM), k, v)

    return jax.shard_map(
        step,
        mesh=mesh,
        in_specs=(P("dp", None, None), P("dp", "sp", None, None), P("dp", "sp", None, None)),
        out_specs=P("dp", None, None),
        check_vma=False,
    )
```

```python
import functools

import jax
import jax.numpy as jnp
from jax import lax
from jax.experimental import pallas as pl
from jax.experimental.pallas import tpu as pltpu
from jax.sharding import PartitionSpec as P

SLOTS = 3
ASIDE = 8
LAG = 9
BATCH = 6
ALONE = 2


def kernel(n, scale, q_hbm, k_hbm, v_hbm, out_ref, q_ref, k_buf, v_buf, parts, ends, q_sem, k_sem, v_sem, send_sem, recv_sem):
    me = lax.axis_index("sp")
    seqs, heads, head = q_ref.shape
    width = heads * head
    last = seqs - 1
    cut = (heads - ASIDE) * head

    def fetch(hbm, buf, sem, s, piece):
        rows = width // sem.shape[1]
        slot, place = lax.rem(s, SLOTS), pl.ds(piece * rows, rows)
        return pltpu.make_async_copy(hbm.at[s, place], buf.at[slot, place], sem.at[slot, piece])

    fetch_k = [functools.partial(fetch, k_hbm, k_buf, k_sem, piece=p) for p in range(k_sem.shape[1])]
    fetch_v = [functools.partial(fetch, v_hbm, v_buf, v_sem, piece=p) for p in range(v_sem.shape[1])]

    for s, copies in (0, fetch_k), (1, fetch_k), (0, fetch_v), (2, fetch_k), (1, fetch_v):
        for copy in copies:
            copy(s).start(priority=1)
    fetch_q = pltpu.make_async_copy(q_hbm, q_ref, q_sem)
    fetch_q.start()

    barrier = pltpu.get_barrier_semaphore()
    for d in range(1, n):
        pl.semaphore_signal(barrier, inc=1, device_id={"sp": lax.rem(me + d, n)})

    def turn(s, fetch, ahead):
        fetch(s).wait()

        @pl.when(s + ahead < seqs)
        def _():
            fetch(s + ahead).start(priority=1)

    def scores_of(s):
        q = q_ref[s]
        row = lax.broadcasted_iota(jnp.int32, (heads, width), 0)
        owner = lax.broadcasted_iota(jnp.int32, (heads, width), 1) // head
        diagonal = jnp.where(owner == row, jnp.concatenate([q] * heads, axis=1), jnp.zeros((), q.dtype))
        return jnp.dot(diagonal, k_buf[lax.rem(s, SLOTS)], preferred_element_type=jnp.float32) * scale

    def weights_of(scores):
        high = jnp.max(scores, -1, keepdims=True)
        weights = jnp.exp(scores - high)
        return weights.astype(v_buf.dtype), jnp.sum(weights, -1, keepdims=True), high

    lane = lax.broadcasted_iota(jnp.int32, (heads, 128), 1)
    row = lax.broadcasted_iota(jnp.int32, (heads, 128), 0)
    per = 128 // head

    def low_of(s, weights):
        every = lax.dot_general(
            weights, v_buf[lax.rem(s, SLOTS), :cut], (((1,), (1,)), ((), ())), preferred_element_type=jnp.float32
        )
        seen = jnp.zeros((heads, 128), jnp.float32)
        for j in range(cut // 128):
            seen = jnp.where(lane // head + per * j == row, every[:, 128 * j : 128 * j + 128], seen)
        return seen + pltpu.roll(seen, head, 1)

    def high_of(s, weights):
        slot = lax.rem(s, SLOTS)
        wide = weights.astype(jnp.float32)
        column = lax.broadcasted_iota(jnp.int32, (head, 128), 1)
        turned = jnp.zeros((head, 128), jnp.float32)
        for h in range(heads - ASIDE, heads):
            terms = [
                v_buf[slot, h * head : (h + 1) * head, t : t + 128].astype(jnp.float32) * wide[h : h + 1, t : t + 128]
                for t in range(0, wide.shape[1], 128)
            ]
            turned = jnp.where(column == h, jnp.sum(functools.reduce(jnp.add, terms), 1, keepdims=True), turned)
        turned = turned.T[:heads]
        return jnp.concatenate([turned, turned], 1)

    def sem_of(s):
        return recv_sem.at[jnp.maximum(s // BATCH, s - (seqs - ALONE) + (seqs - ALONE) // BATCH)]

    def send(place, send_sem, recv_sem):
        for d in sorted(range(1, n), key=lambda d: -min(d, n - d)):
            pltpu.make_async_remote_copy(
                src_ref=place,
                dst_ref=place,
                send_sem=send_sem,
                recv_sem=recv_sem,
                device_id={"sp": lax.rem(me + d, n)},
            ).start()

    def wait_parts(s, count=1):
        place = parts.at[pl.ds(0, n - 1), pl.ds(s, count)]
        pltpu.make_async_copy(place, place, sem_of(s)).wait()

    def shares(tiles, total, high):
        highs = [jnp.broadcast_to(t[:, high : high + 1], t.shape) for t in tiles]
        top = functools.reduce(jnp.maximum, highs)
        factors = [jnp.exp(h - top) for h in highs]
        sums = [f * t for f, t in zip(factors, tiles)]
        whole = functools.reduce(jnp.add, sums)
        return factors, whole, jnp.broadcast_to(whole[:, total : total + 1], whole.shape)

    run = head // 4

    def combine(s):
        _, whole, total = shares([parts[p, s] for p in range(n)], head, head + run)
        out_ref[s] = (whole / total)[:, :head].astype(out_ref.dtype)

    def block(s, state, done=None):
        weights, total, high = state
        for copy in fetch_k:
            turn(s + 1, copy, 2)
        scores = scores_of(s + 1)
        if done is not None:
            combine(done)
        for copy in fetch_v:
            turn(s, copy, 2)
        seen = high_of(s, weights)
        coming = weights_of(scores)
        lanes = low_of(s, weights) + seen
        for first, value in zip(range(head, 2 * head, run), (total, high, coming[1], coming[2])):
            lanes = jnp.where(lane < first, lanes, value)
        parts[me, s] = lanes
        send(parts.at[me, s], send_sem.at[0], sem_of(s))
        return coming

    def later(s, state):
        done = s - 1 - LAG

        @pl.when(lax.rem(done, BATCH) == 0)
        def _():
            wait_parts(done, BATCH)

        return block(s, state, done)

    fetch_q.wait()
    for copy in fetch_k:
        copy(0).wait()
    state = weights_of(scores_of(0))
    pl.semaphore_wait(barrier, n - 1)
    state = lax.fori_loop(0, 1 + LAG, block, state)
    state = lax.fori_loop(1 + LAG, last, later, state)

    for copy in fetch_v:
        copy(last).wait()
    seen = high_of(last, state[0])
    ends[me] = (seen + low_of(last, state[0])).astype(ends.dtype)
    send(ends.at[me], send_sem.at[1], sem_of(last))
    for s in range(last - 1 - LAG, last):
        if s >= seqs - ALONE:
            wait_parts(s)
        elif s % BATCH == 0:
            wait_parts(s, BATCH)
        combine(s)
    factors, _, total = shares([parts[p, last - 1] for p in range(n)], head + 2 * run, head + 3 * run)
    factors = [f / total for f in factors]
    all_ends = ends.at[pl.ds(0, n - 1)]
    pltpu.make_async_copy(all_ends, all_ends, sem_of(last)).wait()
    whole = functools.reduce(jnp.add, [f * ends[p].astype(jnp.float32) for p, f in enumerate(factors)])
    out_ref[last] = whole[:, :head].astype(out_ref.dtype)
    all_parts = parts.at[pl.ds(0, n - 1)]
    pltpu.make_async_copy(all_parts, all_parts, send_sem.at[0]).wait()
    pltpu.make_async_copy(all_ends, all_ends, send_sem.at[1]).wait()


def solution(mesh):
    n = mesh.shape["sp"]

    def step(q, k, v):
        seqs, tokens, heads, head = k.shape
        k = jnp.transpose(k, (0, 2, 3, 1)).reshape(seqs, heads * head, tokens)
        v = jnp.transpose(v, (0, 2, 3, 1)).reshape(seqs, heads * head, tokens)
        return pl.pallas_call(
            functools.partial(kernel, n, head**-0.5),
            out_shape=jax.ShapeDtypeStruct(q.shape, q.dtype),
            in_specs=[pl.BlockSpec(memory_space=pl.ANY)] * 3,
            out_specs=pl.BlockSpec(memory_space=pltpu.VMEM),
            scratch_shapes=[
                pltpu.VMEM(q.shape, q.dtype),
                pltpu.VMEM((SLOTS, heads * head, tokens), k.dtype),
                pltpu.VMEM((SLOTS, heads * head, tokens), v.dtype),
                pltpu.VMEM((n, seqs - 1, heads, 128), jnp.float32),
                pltpu.VMEM((n, heads, 128), q.dtype),
                pltpu.SemaphoreType.DMA,
                pltpu.SemaphoreType.DMA((SLOTS, 1)),
                pltpu.SemaphoreType.DMA((SLOTS, 2)),
                pltpu.SemaphoreType.DMA((2,)),
                pltpu.SemaphoreType.DMA(((seqs - ALONE) // BATCH + ALONE,)),
            ],
            compiler_params=pltpu.CompilerParams(
                collective_id=0, has_side_effects=True, vmem_limit_bytes=30 * 1024 * 1024
            ),
            cost_estimate=pl.CostEstimate(
                flops=4 * seqs * tokens * heads * head,
                bytes_accessed=2 * k.size * k.dtype.itemsize,
                transcendentals=seqs * heads * tokens,
            ),
        )(pltpu.with_memory_space_constraint(q, pltpu.HBM), k, v)

    return jax.shard_map(
        step,
        mesh=mesh,
        in_specs=(P("dp", None, None), P("dp", "sp", None, None), P("dp", "sp", None, None)),
        out_specs=P("dp", None, None),
        check_vma=False,
    )
```
